32 devices in a mesh: srow: 4 (over y, core), scol: 8 (over z, x).
Axes of the slice: x: 2, y: 2, z: 4, core: 2. Of those that a mesh axis runs over, the one named last changes fastest.
Arguments:
- loads: float32 [4, 16, 4, 128], P('srow', 'scol'), may hold values from -6 to 6
- local_inverse: float32 [4, 16, 128, 128], P('srow', 'scol'), as said below
- dirichlet: float32 [4, 16, 128, 128], P('srow', 'scol'), as said below
- corner_coupling: float32 [4, 16, 128], P('srow', 'scol'), may hold values from -4 to 4
- coarse_inverse: float32 [4, 16, 16], P('srow', 'scol'), as said below
- partner: int32 [4, 16, 128], P('srow', 'scol'), may hold values from -1 to 31, as said below
Outputs:
- multipliers: float32 [4, 16, 4, 128], P('srow', 'scol')
- residual: float32 [4, 16, 4, 128], P('srow', 'scol')
The draws below stay inside these ranges and needn't reach their ends.
Inputs may be any that keep to these rules, and one draw needn't show every extreme that they name: `partner`: on each edge of each subdomain the first n entries, for some n of 1 to 32, are the positions 0 to n - 1 in order or reversed, the rest are -1; the two subdomains sharing an edge have the same n and mutually inverse lists. `local_inverse`: each block is symmetric positive definite. `dirichlet`: each block is symmetric positive definite. `coarse_inverse`: each band's matrix is symmetric positive definite.
All inputs are finite; a program needn't handle non-finite values.
Results may differ from the reference program's by a relative error of at most 0.0003.
Values sent between devices are 32-bit elements; how exact they have to be, the bound alone decides.
A program may use at most 64 MiB of HBM per device.

```python
import math
import jax
import jax.numpy as jnp
from jax import lax

NB = 128
SR = 1
SC = 2
NRHS = 4
ITERS = 3
NRS = 4
NCS = 16
BANDS = 4
ORDER = 16
N_SCOL = 8


def symmetric_draw(key, lead, order, diag_low, diag_high):
    key_off = jax.random.fold_in(key, 1)
    key_diag = jax.random.fold_in(key, 2)
    noise = jnp.clip(jax.random.normal(key_off, lead + (order, order), jnp.float32), -4.0, 4.0)
    diagonal = jax.random.uniform(key_diag, lead + (order,), jnp.float32, diag_low, diag_high)
    mixed = (noise + jnp.swapaxes(noise, -1, -2)) * (0.5 / math.sqrt(2.0 * order))
    return mixed + diagonal[..., :, None] * jnp.eye(order, dtype=jnp.float32)


def draw_local_inverse(key, part):
    return symmetric_draw(jax.random.fold_in(key, 5), (NRS, NCS), NB, 1.5, 3.0)


def draw_dirichlet(key, part):
    return symmetric_draw(jax.random.fold_in(key, 7), (NRS, NCS), NB, 1.5, 3.0)


def draw_coarse_inverse(key, part):
    return symmetric_draw(jax.random.fold_in(key, 9), (BANDS,), ORDER, 1.5, 3.0)


def draw_partner(key, part):
    edge_len = NB // 4
    flips = jax.random.randint(jax.random.fold_in(key, 11), (NRS, NCS, 2), 0, 2)
    counts = jax.random.randint(jax.random.fold_in(key, 12), (NRS, NCS, 2), 1, edge_len + 1)
    counts = counts.at[0, 0, 0].set(edge_len).at[0, 0, 1].set(1)
    lengths = jnp.stack([jnp.roll(counts[:, :, 0], 1, axis=1), counts[:, :, 0], jnp.roll(counts[:, :, 1], 1, axis=0), counts[:, :, 1]], axis=-1)
    reversed_edge = jnp.stack([jnp.roll(flips[:, :, 0], 1, axis=1), flips[:, :, 0], jnp.roll(flips[:, :, 1], 1, axis=0), flips[:, :, 1]], axis=-1)
    places = jnp.arange(edge_len, dtype=jnp.int32)
    lengths = lengths[..., None]
    facing = jnp.where(reversed_edge[..., None] == 1, lengths - 1 - places, places)
    listed = jnp.where(places < lengths, facing, -1)
    return listed.reshape(NRS, NCS, NB).astype(jnp.int32)


def block_levels(stream_key, shape, shards, least, high):
    level = 1.0
    for dim, parts in shards:
        draws = jax.random.uniform(jax.random.fold_in(jax.random.fold_in(stream_key, 6), dim), (parts,), jnp.float32, least / len(shards), high / len(shards))
        level = level * jnp.repeat(jnp.exp(draws), shape[dim] // parts).reshape((-1,) + (1,) * (len(shape) - 1 - dim))
    return level


def bell_draw(rng, shape, width, reach, pieces=(), kind=jnp.bfloat16):
    array = jax.random.normal(rng, shape, jnp.float32) * width
    if len(pieces) > 0:
        array = block_levels(rng, shape, pieces, -0.22, 0.18) * array
    return jnp.clip(array, min=-reach, max=reach).astype(kind)


def setup_inputs(seed: int = 0) -> dict:
    arg_keys = jax.random.split(jax.random.key(seed), 7)
    return {
        "loads": bell_draw(arg_keys[0], (NRS, NCS, NRHS, NB), 1.0, 6.0, ((0, 4), (1, 8)), jnp.float32),
        "local_inverse": draw_local_inverse(jax.random.fold_in(arg_keys[6], 71), 0),
        "dirichlet": draw_dirichlet(jax.random.fold_in(arg_keys[6], 71), 0),
        "corner_coupling": bell_draw(arg_keys[3], (NRS, NCS, NB), (3.0 * NB ** -0.5), 4.0, ((0, 4), (1, 8)), jnp.float32),
        "coarse_inverse": draw_coarse_inverse(jax.random.fold_in(arg_keys[6], 71), 0),
        "partner": draw_partner(jax.random.fold_in(arg_keys[6], 71), 0),
    }


precise = lax.Precision.HIGHEST


def jump(values, partner):
    edge_len = NB // 4
    west_side = jnp.roll(values, 1, axis=1)[..., edge_len:2 * edge_len]
    east_side = jnp.roll(values, -1, axis=1)[..., 0:edge_len]
    south_side = jnp.roll(values, 1, axis=0)[..., 3 * edge_len:]
    north_side = jnp.roll(values, -1, axis=0)[..., 2 * edge_len:3 * edge_len]
    facing = jnp.concatenate([west_side, east_side, south_side, north_side], axis=-1)
    offset = (jnp.arange(NB, dtype=jnp.int32) // edge_len) * edge_len
    position = (jnp.clip(partner, 0, edge_len - 1) + offset).astype(jnp.int32)
    position = jnp.broadcast_to(position[:, :, None, :], values.shape)
    picked = jnp.take_along_axis(facing, position, axis=-1)
    return jnp.where(partner[:, :, None, :] >= 0, values - picked, jnp.zeros_like(values))


def jump_transposed(values, partner):
    return jump(values, partner)


def apply_inverse(values, local_inverse, corner_coupling, coarse_inverse):
    blocks = jnp.einsum("ijab,ijrb->ijra", local_inverse, values, precision=precise)
    coarse_in = jnp.einsum("ijb,ijrb->ijr", corner_coupling, values, precision=precise)
    banded = coarse_in.reshape(BANDS, SR, N_SCOL, SC, NRHS).transpose(0, 2, 1, 3, 4).reshape(BANDS, ORDER, NRHS)
    solved = jnp.einsum("bxy,byr->bxr", coarse_inverse, banded, precision=precise)
    coarse_out = solved.reshape(BANDS, N_SCOL, SR, SC, NRHS).transpose(0, 2, 1, 3, 4).reshape(NRS, NCS, NRHS)
    return blocks + corner_coupling[:, :, None, :] * coarse_out[..., None]


def inner(left, right):
    return jnp.sum(left * right, axis=(0, 1, 3))


def scaled(coef, values):
    return coef[None, None, :, None] * values


def reference(loads, local_inverse, dirichlet, corner_coupling, coarse_inverse, partner):
    def operator(values):
        spread = jump_transposed(values, partner)
        return jump(apply_inverse(spread, local_inverse, corner_coupling, coarse_inverse), partner)

    def precond(values):
        spread = jump_transposed(values, partner)
        return jump(jnp.einsum("ijab,ijrb->ijra", dirichlet, spread, precision=precise), partner)

    right = operator(loads)
    multipliers = jnp.zeros_like(right)
    residual = right
    precon = precond(residual)
    search = precon
    gamma = inner(residual, precon)
    for iteration in range(ITERS):
        image = operator(search)
        step_size = gamma / inner(search, image)
        multipliers = multipliers + scaled(step_size, search)
        residual = residual - scaled(step_size, image)
        if iteration + 1 < ITERS:
            precon = precond(residual)
            gamma_new = inner(residual, precon)
            search = precon + scaled(gamma_new / gamma, search)
            gamma = gamma_new
    return multipliers, residual
```

```python
import functools

import jax
import jax.numpy as jnp
from jax import lax
from jax.experimental import pallas as pl
from jax.experimental.pallas import tpu as pltpu
from jax.sharding import PartitionSpec as P

ITERS = 3
MESH = pl.DeviceIdType.MESH
precise = lax.Precision.HIGHEST
NEAR = ((0, 0), (0, 1), (0, -1), (1, 0), (-1, 0))
FAR = ((1, 1), (1, -1), (-1, 1), (-1, -1), (2, 0), (-2, 0))
UNROLL = 64


def slot_list(nr, nc):
    near, slots = [], []
    for offsets, out in ((NEAR, near), (FAR, None)):
        for di, dj in offsets:
            off = (di % nr, dj % nc)
            if off not in slots:
                slots.append(off)
                if out is not None:
                    out.append(off)
    return near, slots


def kernel(nr, nc, near, slots, sc, nrhs, loads, cpl, cinv, part, linv, dirich, m_out, r_out,
           lbuf, dbuf, loads_n, part_n, cpl_n, kt, ub, qb,
           local_sem, k_send, k_recv, c_send, c_recv, l_send, l_recv, p_send, p_recv, d_send, d_recv,
           u_send, u_recv, q_send, q_recv):
    rows, width = loads.shape
    edge = width // 4
    ndev = nr * nc
    ncols = nc * sc
    lanes = kt.shape[-1]
    i, j = lax.axis_index("srow"), lax.axis_index("scol")

    def target(di, dj):
        return (lax.rem(i - di + nr, nr), lax.rem(j - dj + nc, nc))

    def others(step):
        if ndev <= UNROLL:
            for k in range(1, ndev):
                step(k, k // nc, k % nc)
        else:
            @pl.loop(1, ndev)
            def _(k):
                step(k, lax.div(k, nc), lax.rem(k, nc))

    fetch_l = pltpu.make_async_copy(linv, lbuf, local_sem.at[0])
    fetch_d = pltpu.make_async_copy(dirich, dbuf.at[0], local_sem.at[1])
    fetch_l.start()
    fetch_d.start()

    barrier = pltpu.get_barrier_semaphore()

    def greet(k, di, dj):
        pl.semaphore_signal(barrier, inc=1, device_id=target(di, dj), device_id_type=MESH)

    others(greet)

    row = lax.broadcasted_iota(jnp.int32, (rows, width), 0)
    lane = lax.broadcasted_iota(jnp.int32, (rows, width), 1)
    wrow = lax.broadcasted_iota(jnp.int32, (rows, lanes), 0)
    wlane = lax.broadcasted_iota(jnp.int32, (rows, lanes), 1)
    wrhs = lax.rem(wrow, nrhs)
    wsub = lax.div(wrow, nrhs)
    of_rhs = lax.div(wlane, ncols) == wrhs
    gamma_lane = wlane == nrhs * ncols + wrhs
    curve_lane = wlane == nrhs * ncols + nrhs + wrhs

    def spread(block):
        out = jnp.broadcast_to(block[0:1], (rows, block.shape[1]))
        which = lax.div(lax.broadcasted_iota(jnp.int32, out.shape, 0), nrhs)
        for s in range(1, sc):
            out = jnp.where(which == s, jnp.broadcast_to(block[s : s + 1], out.shape), out)
        return out

    def place(dj):
        column = lax.rem(j + dj, nc) * sc
        return wlane == wrhs * ncols + column + wsub

    tile_lane = lax.broadcasted_iota(jnp.int32, (ncols, lanes), 1)
    tile_row = lax.broadcasted_iota(jnp.int32, (ncols, lanes), 0)
    tiler = jnp.where(lax.rem(tile_lane, ncols) == tile_row, 1.0, 0.0)
    tiled = jnp.dot(spread(cinv[...]), tiler, precision=precise, preferred_element_type=jnp.float32)
    kt[0] = jnp.where(of_rhs, tiled, 0.0)

    pl.semaphore_wait(barrier, ndev - 1)

    def remote(src, dst, send, recv, off):
        copy = pltpu.make_async_remote_copy(
            src_ref=src, dst_ref=dst, send_sem=send, recv_sem=recv,
            device_id=target(*off), device_id_type=MESH)
        copy.start()
        return copy

    load_copies = [remote(loads, loads_n.at[n], l_send.at[n], l_recv.at[n], near[n]) for n in range(1, len(near))]
    part_copies = [remote(part, part_n.at[n], p_send.at[n], p_recv.at[n], near[n]) for n in range(1, len(near))]
    cpl_copies = [remote(cpl, cpl_n.at[n], c_send.at[n], c_recv.at[n], slots[n]) for n in range(1, len(slots))]
    east_off, west_off = (0, 1 % nc), (0, nc - 1)
    d_copies = []
    for n in range(1, len(near)):
        if near[n] == east_off:
            src, dst = dirich.at[pl.ds(0, 1)], dbuf.at[n, pl.ds(0, 1)]
        elif near[n] == west_off:
            src, dst = dirich.at[pl.ds(sc - 1, 1)], dbuf.at[n, pl.ds(sc - 1, 1)]
        else:
            src, dst = dirich, dbuf.at[n]
        d_copies.append((src, dst, d_send.at[n], d_recv.at[n], near[n]))

    def send_k(k, di, dj):
        remote(kt.at[0], kt.at[k], k_send, k_recv, (di, dj))

    others(send_k)
    d_copies = [remote(*args) for args in d_copies]

    def index_of(block):
        partner = spread(block)
        position = jnp.clip(partner, 0, edge - 1) + (edge * (1 - 2 * lax.rem(lax.div(lane, edge), 2)) + lax.div(lane, edge) * edge)
        return position, partner >= 0

    def jump(mine, west_tile, east_tile, south, north, lookup):
        position, active = lookup
        west = jnp.where(row < nrhs, pltpu.roll(west_tile, nrhs, 0), pltpu.roll(mine, nrhs, 0))
        east = jnp.where(row >= rows - nrhs, pltpu.roll(east_tile, rows - nrhs, 0), pltpu.roll(mine, rows - nrhs, 0))
        side = lax.div(lane, edge)
        comb = jnp.where(side == 0, east, jnp.where(side == 1, west, jnp.where(side == 2, north, south)))
        facing = jnp.take_along_axis(comb, position, axis=1, mode="promise_in_bounds")
        return jnp.where(active, mine - facing, 0.0)

    def slot_of(di, dj):
        off = (di % nr, dj % nc)
        return slots.index(off) if off in slots else None

    def jump_at(tiles, di, dj, lookup):
        def tile(a, b):
            n = slot_of(a, b)
            return tiles[n] if n is not None and n in tiles else tiles[slot_of(di, dj)]
        return jump(tiles[slot_of(di, dj)], tile(di, dj - 1), tile(di, dj + 1), tile(di - 1, dj), tile(di + 1, dj), lookup)

    def multiply(values, blocks):
        out = None
        for s, block in blocks:
            term = jnp.dot(values, block, precision=precise, preferred_element_type=jnp.float32)
            out = term if out is None else jnp.where(lax.div(row, nrhs) == s, term, out)
        return out

    def lane_sum(values):
        return jnp.sum(values, axis=1, keepdims=True)

    coupling = spread(cpl[...])
    own_place = place(0)

    def publish(rd, values, dots, wide):
        u = multiply(values, [(s, lbuf[s]) for s in range(sc)])
        ub[rd, 0] = u
        count = len(slots) if wide else len(near)
        for n in range(1, count):
            remote(ub.at[rd, 0], ub.at[rd, n], u_send.at[rd], u_recv.at[rd], slots[n])
        message = jnp.where(own_place, lane_sum(coupling * values), 0.0)
        if dots is not None:
            gamma, factor = dots
            message = jnp.where(gamma_lane, lane_sum(gamma), message)
            message = jnp.where(curve_lane, lane_sum(factor * u), message)
        qb[rd, 0] = jnp.sum(message, axis=0, keepdims=True)

        def send_q(k, di, dj):
            remote(qb.at[rd, 0], qb.at[rd, k], q_send.at[rd], q_recv.at[rd], (di, dj))

        others(send_q)
        return count

    def collect(rd, count, want_dots):
        bytes_q = qb.at[rd, pl.ds(1, ndev - 1)]
        pltpu.make_async_copy(bytes_q, bytes_q, q_recv.at[rd]).wait()
        band = [jnp.broadcast_to(jnp.sum(qb[rd, pl.ds(d * nc, nc)], axis=0), (rows, lanes)) for d in range(nr)]
        cols = {}

        def column(k, d):
            return lane_sum(band[d] * kt[k])

        gamma = curve = None
        if want_dots:
            cross = jnp.zeros((rows, lanes), jnp.float32)
            for d in range(nr):
                total = jnp.zeros((rows, lanes), jnp.float32)
                if ndev <= UNROLL:
                    for e in range(nc):
                        cols[(d, e)] = column(d * nc + e, d)
                        total = total + jnp.where(place(e), cols[(d, e)], 0.0)
                else:
                    def add(e, total):
                        return total + jnp.where(place(e), column(d * nc + e, d), 0.0)
                    total = lax.fori_loop(0, nc, add, total)
                cross = cross + total * band[d]
            everything = functools.reduce(jnp.add, band)
            crossed = jnp.broadcast_to(jnp.sum(cross, axis=0, keepdims=True), (rows, lanes))
            curve = lane_sum(jnp.where(of_rhs, crossed, 0.0) + jnp.where(curve_lane, everything, 0.0))
            gamma = lane_sum(jnp.where(gamma_lane, everything, 0.0))
        bytes_u = ub.at[rd, pl.ds(1, count - 1)]
        pltpu.make_async_copy(bytes_u, bytes_u, u_recv.at[rd]).wait()
        tiles = {}
        for n in range(count):
            off = slots[n]
            if off not in cols:
                cols[off] = column(off[0] * nc + off[1], off[0])
            tiles[n] = ub[rd, n] + couplings[n] * cols[off]
        return tiles, gamma, curve

    for n, copy in enumerate(load_copies):
        copy.wait_recv()
    own_lookup = index_of(part[...])
    load_tiles = {n: (loads[...] if n == 0 else loads_n[n]) for n in range(len(near))}
    start = jump_at(load_tiles, 0, 0, own_lookup)
    fetch_l.wait()
    count = publish(0, start, None, True)

    for copy in part_copies:
        copy.wait_recv()
    for copy in cpl_copies:
        copy.wait_recv()
    lookups = [own_lookup] + [index_of(part_n[n]) for n in range(1, len(near))]
    couplings = [coupling] + [spread(cpl_n[n]) for n in range(1, len(slots))]
    bytes_k = kt.at[pl.ds(1, ndev - 1)]
    pltpu.make_async_copy(bytes_k, bytes_k, k_recv).wait()
    tiles, _, _ = collect(0, count, False)
    residual = [jump_at(tiles, *near[n], lookups[n]) for n in range(len(near))]
    fetch_d.wait()
    for copy in d_copies:
        copy.wait_recv()

    multipliers = jnp.zeros((rows, width), jnp.float32)
    search = along = gamma = step_size = None
    for iteration in range(ITERS):
        rd = iteration + 1
        last = rd == ITERS
        weighted = {}
        for n in range(len(near)):
            if near[n] == east_off:
                blocks = [(0, dbuf[n, 0])]
            elif near[n] == west_off:
                blocks = [(sc - 1, dbuf[n, sc - 1])]
            else:
                blocks = [(s, dbuf[n, s]) for s in range(sc)]
            weighted[n] = multiply(2.0 * residual[n], blocks)
        precon = jump_at(weighted, 0, 0, own_lookup)
        doubled = 2.0 * precon
        count = publish(rd, doubled, (residual[0] * precon, doubled), not last)
        tiles, gamma_new, curve = collect(rd, count, True)
        kept = 1 if last else len(near)
        image = [jump_at(tiles, *near[n], lookups[n]) for n in range(kept)]
        if iteration == 0:
            step_size = gamma_new / curve
            search, along = precon, image
        else:
            ratio = gamma_new / gamma
            step_size = gamma_new / (curve - ratio * gamma_new / step_size)
            search = precon + ratio * search
            along = [image[n] + ratio * along[n] for n in range(kept)]
        gamma = gamma_new
        multipliers = multipliers + step_size * search
        residual = [residual[n] - step_size * along[n] for n in range(kept)]
    m_out[...] = multipliers
    r_out[...] = residual[0]

    for copy in load_copies + part_copies + cpl_copies + d_copies:
        copy.wait_send()
    pltpu.make_async_copy(bytes_k, bytes_k, k_send).wait()
    for rd in range(ITERS + 1):
        bytes_q = qb.at[rd, pl.ds(1, ndev - 1)]
        pltpu.make_async_copy(bytes_q, bytes_q, q_send.at[rd]).wait()
        sent = (len(near) if rd == ITERS else len(slots)) - 1
        bytes_u = ub.at[rd, pl.ds(1, sent)]
        pltpu.make_async_copy(bytes_u, bytes_u, u_send.at[rd]).wait()


def solution(mesh):
    nr, nc = mesh.shape["srow"], mesh.shape["scol"]
    near, slots = slot_list(nr, nc)

    def body(loads, local_inverse, dirichlet, corner_coupling, coarse_inverse, partner):
        sr, sc, nrhs, width = loads.shape
        rows = sr * sc * nrhs
        ndev = nr * nc
        lanes = -(-(nrhs * nc * sc + 2 * nrhs) // 128) * 128
        dma = pltpu.SemaphoreType.DMA
        f32 = jnp.float32
        vmem = pl.BlockSpec(memory_space=pltpu.VMEM)
        hbm = pl.BlockSpec(memory_space=pl.ANY)
        tile = jax.ShapeDtypeStruct((rows, width), f32)
        rounds = ITERS + 1
        m, r = pl.pallas_call(
            functools.partial(kernel, nr, nc, near, slots, sc, nrhs),
            out_shape=(tile, tile),
            in_specs=[vmem, vmem, vmem, vmem, hbm, hbm],
            out_specs=(vmem, vmem),
            scratch_shapes=[
                pltpu.VMEM((sc, width, width), f32),
                pltpu.VMEM((len(near), sc, width, width), f32),
                pltpu.VMEM((len(near), rows, width), f32),
                pltpu.VMEM((len(near), sc, width), jnp.int32),
                pltpu.VMEM((len(slots), sc, width), f32),
                pltpu.VMEM((ndev, rows, lanes), f32),
                pltpu.VMEM((rounds, len(slots), rows, width), f32),
                pltpu.VMEM((rounds, ndev, 1, lanes), f32),
                dma((2,)), dma, dma,
                dma((len(slots),)), dma((len(slots),)),
                dma((len(near),)), dma((len(near),)),
                dma((len(near),)), dma((len(near),)),
                dma((len(near),)), dma((len(near),)),
                dma((rounds,)), dma((rounds,)),
                dma((rounds,)), dma((rounds,)),
            ],
            compiler_params=pltpu.CompilerParams(collective_id=0, has_side_effects=True),
        )(
            loads.reshape(rows, width),
            corner_coupling.reshape(sc, width),
            coarse_inverse.reshape(sc, coarse_inverse.shape[-1]),
            partner.reshape(sc, width),
            local_inverse.reshape(sc, width, width),
            dirichlet.reshape(sc, width, width),
        )
        return m.reshape(loads.shape), r.reshape(loads.shape)

    return jax.shard_map(
        body,
        mesh=mesh,
        in_specs=(
            P("srow", "scol", None, None),
            P("srow", "scol", None, None),
            P("srow", "scol", None, None),
            P("srow", "scol", None),
            P("srow", "scol", None),
            P("srow", "scol", None),
        ),
        out_specs=(P("srow", "scol", None, None), P("srow", "scol", None, None)),
        check_vma=False,
    )
```

```python
import functools

import jax
import jax.numpy as jnp
from jax import lax
from jax.experimental import pallas as pl
from jax.experimental.pallas import tpu as pltpu
from jax.sharding import PartitionSpec as P

ITERS = 3
MESH = pl.DeviceIdType.MESH
precise = lax.Precision.HIGHEST
NEAR = ((0, 0), (0, 1), (0, -1), (1, 0), (-1, 0))
FAR = ((1, 1), (1, -1), (-1, 1), (-1, -1), (2, 0), (-2, 0))
UNROLL = 64


def slot_list(nr, nc):
    near, slots = [], []
    for offsets, out in ((NEAR, near), (FAR, None)):
        for di, dj in offsets:
            off = (di % nr, dj % nc)
            if off not in slots:
                slots.append(off)
                if out is not None:
                    out.append(off)
    return near, slots


def kernel(nr, nc, near, slots, sc, nrhs, loads_in, cpl_in, cinv_in, part_in, linv, dirich, out,
           loads, cpl, cinv, part, lbuf, dbuf, lpair, dpair, loads_n, part_n, cpl_n, kt, ub, qb,
           local_sem, k_send, k_recv, c_send, c_recv, l_send, l_recv, p_send, p_recv, d_send, d_recv,
           u_send, u_recv, q_send, q_recv):
    rows, width = loads.shape
    edge = width // 4
    ndev = nr * nc
    ncols = nc * sc
    lanes = kt.shape[-1]
    i, j = lax.axis_index("srow"), lax.axis_index("scol")

    def target(di, dj):
        return (lax.rem(i - di + nr, nr), lax.rem(j - dj + nc, nc))

    def others(step):
        if ndev <= UNROLL:
            for k in range(1, ndev):
                step(k, k // nc, k % nc)
        else:
            @pl.loop(1, ndev)
            def _(k):
                step(k, lax.div(k, nc), lax.rem(k, nc))

    barrier = pltpu.get_barrier_semaphore()

    def greet(k, di, dj):
        pl.semaphore_signal(barrier, inc=1, device_id=target(di, dj), device_id_type=MESH)

    others(greet)

    fetches = [
        pltpu.make_async_copy(src, dst, local_sem.at[n])
        for n, (src, dst) in enumerate((
            (cinv_in, cinv), (loads_in, loads), (cpl_in, cpl), (part_in, part),
            (linv, lbuf), (dirich, dbuf.at[0]),
        ))
    ]
    for fetch in fetches:
        fetch.start()

    row = lax.broadcasted_iota(jnp.int32, (rows, width), 0)
    lane = lax.broadcasted_iota(jnp.int32, (rows, width), 1)
    wrow = lax.broadcasted_iota(jnp.int32, (rows, lanes), 0)
    wlane = lax.broadcasted_iota(jnp.int32, (rows, lanes), 1)
    wrhs = lax.rem(wrow, nrhs)
    wsub = lax.div(wrow, nrhs)
    of_rhs = lax.div(wlane, ncols) == wrhs
    gamma_lane = wlane == nrhs * ncols + wrhs
    curve_lane = wlane == nrhs * ncols + nrhs + wrhs

    def spread(block):
        out = jnp.broadcast_to(block[0:1], (rows, block.shape[1]))
        which = lax.div(lax.broadcasted_iota(jnp.int32, out.shape, 0), nrhs)
        for s in range(1, sc):
            out = jnp.where(which == s, jnp.broadcast_to(block[s : s + 1], out.shape), out)
        return out

    def place(dj):
        column = lax.rem(j + dj, nc) * sc
        return wlane == wrhs * ncols + column + wsub

    def index_of(block):
        partner = spread(block)
        position = jnp.clip(partner, 0, edge - 1) + (edge * (1 - 2 * lax.rem(lax.div(lane, edge), 2)) + lax.div(lane, edge) * edge)
        return position, partner >= 0

    def split(values):
        high = values.astype(jnp.bfloat16)
        return high, (values - high.astype(jnp.float32)).astype(jnp.bfloat16)

    def split_into(pair, blocks):
        for s, block in enumerate(blocks):
            high, low = split(block)
            pair[s * width : (s + 1) * width, 0:width] = high
            pair[s * width : (s + 1) * width, width : 2 * width] = low

    tile_lane = lax.broadcasted_iota(jnp.int32, (ncols, lanes), 1)
    tile_row = lax.broadcasted_iota(jnp.int32, (ncols, lanes), 0)
    tiler = jnp.where(lax.rem(tile_lane, ncols) == tile_row, 1.0, 0.0)
    for fetch in fetches[:4]:
        fetch.wait()
    tiled = jnp.dot(spread(cinv[...]), tiler, precision=precise, preferred_element_type=jnp.float32)
    kt[0] = jnp.where(of_rhs, tiled, 0.0)

    own_position, own_active = index_of(part[...])
    coupling = spread(cpl[...])
    own_place = place(0)
    fetches[4].wait()
    split_into(lpair, [lbuf[s] for s in range(sc)])

    pl.semaphore_wait(barrier, ndev - 1)

    def remote(src, dst, send, recv, off):
        copy = pltpu.make_async_remote_copy(
            src_ref=src, dst_ref=dst, send_sem=send, recv_sem=recv,
            device_id=target(*off), device_id_type=MESH)
        copy.start()
        return copy

    load_copies = [remote(loads, loads_n.at[n], l_send.at[n], l_recv.at[n], near[n]) for n in range(1, len(near))]
    part_copies = [remote(part, part_n.at[n], p_send.at[n], p_recv.at[n], near[n]) for n in range(1, len(near))]
    cpl_copies = [remote(cpl, cpl_n.at[n], c_send.at[n], c_recv.at[n], slots[n]) for n in range(1, len(slots))]
    east_off, west_off = (0, 1 % nc), (0, nc - 1)
    d_copies = []
    for n in range(1, len(near)):
        if near[n] == east_off:
            src, dst = dirich.at[pl.ds(0, 1)], dbuf.at[n, pl.ds(0, 1)]
        elif near[n] == west_off:
            src, dst = dirich.at[pl.ds(sc - 1, 1)], dbuf.at[n, pl.ds(sc - 1, 1)]
        else:
            src, dst = dirich, dbuf.at[n]
        d_copies.append((src, dst, d_send.at[n], d_recv.at[n], near[n]))

    def send_k(k, di, dj):
        remote(kt.at[0], kt.at[k], k_send, k_recv, (di, dj))

    others(send_k)
    d_copies = [remote(*args) for args in d_copies]

    def jump(mine, west_tile, east_tile, south, north, lookup):
        position, active = lookup
        west = jnp.where(row < nrhs, pltpu.roll(west_tile, nrhs, 0), pltpu.roll(mine, nrhs, 0))
        east = jnp.where(row >= rows - nrhs, pltpu.roll(east_tile, rows - nrhs, 0), pltpu.roll(mine, rows - nrhs, 0))
        side = lax.div(lane, edge)
        comb = jnp.where(side == 0, east, jnp.where(side == 1, west, jnp.where(side == 2, north, south)))
        facing = jnp.take_along_axis(comb, position, axis=1, mode="promise_in_bounds")
        return jnp.where(active, mine - facing, 0.0)

    def slot_of(di, dj):
        off = (di % nr, dj % nc)
        return slots.index(off) if off in slots else None

    def jump_at(tiles, di, dj, lookup):
        def tile(a, b):
            n = slot_of(a, b)
            return tiles[n] if n is not None and n in tiles else tiles[slot_of(di, dj)]
        return jump(tiles[slot_of(di, dj)], tile(di, dj - 1), tile(di, dj + 1), tile(di - 1, dj), tile(di + 1, dj), lookup)

    def multiply(values, pair, count):
        high, low = split(values)
        stacked = jnp.concatenate([high.astype(jnp.float32), low.astype(jnp.float32)], axis=0)
        sub = lax.rem(lax.div(lax.broadcasted_iota(jnp.int32, stacked.shape, 0), nrhs), sc)
        wide = jnp.concatenate(
            [jnp.where(sub == (s if s < count - 1 else sc - 1), stacked, 0.0) for s in range(count)], axis=1)
        product = jnp.dot(wide.astype(jnp.bfloat16), pair, preferred_element_type=jnp.float32)
        return (product[0:rows, 0:width] + product[rows:, 0:width]) + (product[0:rows, width:] + product[rows:, width:])

    def lane_sum(values):
        return jnp.sum(values, axis=1, keepdims=True)

    def publish(rd, values, dots, wide):
        u = multiply(values, lpair[...], sc)
        ub[rd, 0] = u
        count = len(slots) if wide else len(near)
        for n in range(1, count):
            remote(ub.at[rd, 0], ub.at[rd, n], u_send.at[rd], u_recv.at[rd], slots[n])
        message = jnp.where(own_place, lane_sum(coupling * values), 0.0)
        if dots is not None:
            gamma, factor = dots
            message = jnp.where(gamma_lane, lane_sum(gamma), message)
            message = jnp.where(curve_lane, lane_sum(factor * u), message)
        qb[rd, 0] = jnp.sum(message, axis=0, keepdims=True)

        def send_q(k, di, dj):
            remote(qb.at[rd, 0], qb.at[rd, k], q_send.at[rd], q_recv.at[rd], (di, dj))

        others(send_q)
        return count

    def collect(rd, count, want_dots):
        bytes_q = qb.at[rd, pl.ds(1, ndev - 1)]
        pltpu.make_async_copy(bytes_q, bytes_q, q_recv.at[rd]).wait()
        band = [jnp.broadcast_to(jnp.sum(qb[rd, pl.ds(d * nc, nc)], axis=0), (rows, lanes)) for d in range(nr)]
        cols = {}

        def column(k, d):
            return lane_sum(band[d] * kt[k])

        gamma = curve = None
        if want_dots:
            cross = jnp.zeros((rows, lanes), jnp.float32)
            for d in range(nr):
                total = jnp.zeros((rows, lanes), jnp.float32)
                if ndev <= UNROLL:
                    for e in range(nc):
                        cols[(d, e)] = column(d * nc + e, d)
                        total = total + jnp.where(place(e), cols[(d, e)], 0.0)
                else:
                    def add(e, total):
                        return total + jnp.where(place(e), column(d * nc + e, d), 0.0)
                    total = lax.fori_loop(0, nc, add, total)
                cross = cross + total * band[d]
            everything = functools.reduce(jnp.add, band)
            crossed = jnp.broadcast_to(jnp.sum(cross, axis=0, keepdims=True), (rows, lanes))
            curve = lane_sum(jnp.where(of_rhs, crossed, 0.0) + jnp.where(curve_lane, everything, 0.0))
            gamma = lane_sum(jnp.where(gamma_lane, everything, 0.0))
        bytes_u = ub.at[rd, pl.ds(1, count - 1)]
        pltpu.make_async_copy(bytes_u, bytes_u, u_recv.at[rd]).wait()
        tiles = {}
        for n in range(count):
            off = slots[n]
            if off not in cols:
                cols[off] = column(off[0] * nc + off[1], off[0])
            tiles[n] = ub[rd, n] + couplings[n] * cols[off]
        return tiles, gamma, curve

    for n, copy in enumerate(load_copies):
        copy.wait_recv()
    own_lookup = (own_position, own_active)
    load_tiles = {n: (loads[...] if n == 0 else loads_n[n]) for n in range(len(near))}
    start = jump_at(load_tiles, 0, 0, own_lookup)
    count = publish(0, start, None, True)

    for copy in part_copies:
        copy.wait_recv()
    for copy in cpl_copies:
        copy.wait_recv()
    lookups = [own_lookup] + [index_of(part_n[n]) for n in range(1, len(near))]
    couplings = [coupling] + [spread(cpl_n[n]) for n in range(1, len(slots))]
    bytes_k = kt.at[pl.ds(1, ndev - 1)]
    pltpu.make_async_copy(bytes_k, bytes_k, k_recv).wait()
    fetches[5].wait()
    for copy in d_copies:
        copy.wait_recv()
    east, west = near.index(east_off), near.index(west_off)
    upright = [n for n in range(len(near)) if n not in (east, west)]
    for n in upright:
        split_into(dpair.at[n], [dbuf[n, s] for s in range(sc)])
    split_into(dpair.at[east], [dbuf[east, 0], dbuf[west, sc - 1]])
    tiles, _, _ = collect(0, count, False)
    residual = [jump_at(tiles, *near[n], lookups[n]) for n in range(len(near))]

    multipliers = jnp.zeros((rows, width), jnp.float32)
    search = along = gamma = step_size = None
    for iteration in range(ITERS):
        rd = iteration + 1
        last = rd == ITERS
        weighted = {}
        for n in upright:
            weighted[n] = multiply(2.0 * residual[n], dpair[n], sc)
        beside = jnp.where(row < nrhs, residual[east], residual[west])
        weighted[east] = weighted[west] = multiply(2.0 * beside, dpair[east, pl.ds(0, 2 * width)], 2)
        precon = jump_at(weighted, 0, 0, own_lookup)
        doubled = 2.0 * precon
        count = publish(rd, doubled, (residual[0] * precon, doubled), not last)
        tiles, gamma_new, curve = collect(rd, count, True)
        kept = 1 if last else len(near)
        image = [jump_at(tiles, *near[n], lookups[n]) for n in range(kept)]
        if iteration == 0:
            step_size = gamma_new / curve
            search, along = precon, image
        else:
            ratio = gamma_new / gamma
            step_size = gamma_new / (curve - ratio * gamma_new / step_size)
            search = precon + ratio * search
            along = [image[n] + ratio * along[n] for n in range(kept)]
        gamma = gamma_new
        multipliers = multipliers + step_size * search
        residual = [residual[n] - step_size * along[n] for n in range(kept)]
    out[0] = multipliers
    out[1] = residual[0]

    for copy in load_copies + part_copies + cpl_copies + d_copies:
        copy.wait_send()
    pltpu.make_async_copy(bytes_k, bytes_k, k_send).wait()
    for rd in range(ITERS + 1):
        bytes_q = qb.at[rd, pl.ds(1, ndev - 1)]
        pltpu.make_async_copy(bytes_q, bytes_q, q_send.at[rd]).wait()
        sent = (len(near) if rd == ITERS else len(slots)) - 1
        bytes_u = ub.at[rd, pl.ds(1, sent)]
        pltpu.make_async_copy(bytes_u, bytes_u, u_send.at[rd]).wait()


def solution(mesh):
    nr, nc = mesh.shape["srow"], mesh.shape["scol"]
    near, slots = slot_list(nr, nc)

    def body(loads, local_inverse, dirichlet, corner_coupling, coarse_inverse, partner):
        sr, sc, nrhs, width = loads.shape
        rows = sr * sc * nrhs
        ndev = nr * nc
        lanes = -(-(nrhs * nc * sc + 2 * nrhs) // 128) * 128
        dma = pltpu.SemaphoreType.DMA
        f32 = jnp.float32
        vmem = pl.BlockSpec(memory_space=pltpu.VMEM)
        hbm = pl.BlockSpec(memory_space=pl.ANY)
        rounds = ITERS + 1
        out = pl.pallas_call(
            functools.partial(kernel, nr, nc, near, slots, sc, nrhs),
            out_shape=jax.ShapeDtypeStruct((2, rows, width), f32),
            in_specs=[hbm] * 6,
            out_specs=vmem,
            scratch_shapes=[
                pltpu.VMEM((rows, width), f32),
                pltpu.VMEM((sc, width), f32),
                pltpu.VMEM((sc, coarse_inverse.shape[-1]), f32),
                pltpu.VMEM((sc, width), jnp.int32),
                pltpu.VMEM((sc, width, width), f32),
                pltpu.VMEM((len(near), sc, width, width), f32),
                pltpu.VMEM((sc * width, 2 * width), jnp.bfloat16),
                pltpu.VMEM((len(near), sc * width, 2 * width), jnp.bfloat16),
                pltpu.VMEM((len(near), rows, width), f32),
                pltpu.VMEM((len(near), sc, width), jnp.int32),
                pltpu.VMEM((len(slots), sc, width), f32),
                pltpu.VMEM((ndev, rows, lanes), f32),
                pltpu.VMEM((rounds, len(slots), rows, width), f32),
                pltpu.VMEM((rounds, ndev, 1, lanes), f32),
                dma((6,)), dma, dma,
                dma((len(slots),)), dma((len(slots),)),
                dma((len(near),)), dma((len(near),)),
                dma((len(near),)), dma((len(near),)),
                dma((len(near),)), dma((len(near),)),
                dma((rounds,)), dma((rounds,)),
                dma((rounds,)), dma((rounds,)),
            ],
            compiler_params=pltpu.CompilerParams(collective_id=0, has_side_effects=True),
        )(
            loads.reshape(rows, width),
            corner_coupling.reshape(sc, width),
            coarse_inverse.reshape(sc, coarse_inverse.shape[-1]),
            partner.reshape(sc, width),
            local_inverse.reshape(sc, width, width),
            dirichlet.reshape(sc, width, width),
        )
        return out[0].reshape(loads.shape), out[1].reshape(loads.shape)

    return jax.shard_map(
        body,
        mesh=mesh,
        in_specs=(
            P("srow", "scol", None, None),
            P("srow", "scol", None, None),
            P("srow", "scol", None, None),
            P("srow", "scol", None),
            P("srow", "scol", None),
            P("srow", "scol", None),
        ),
        out_specs=(P("srow", "scol", None, None), P("srow", "scol", None, None)),
        check_vma=False,
    )
```

```python
import functools

import jax
import jax.numpy as jnp
from jax import lax
from jax.experimental import pallas as pl
from jax.experimental.pallas import tpu as pltpu
from jax.sharding import PartitionSpec as P

ITERS = 3
MESH = pl.DeviceIdType.MESH
precise = lax.Precision.HIGHEST
NEAR = ((0, 0), (0, 1), (0, -1), (1, 0), (-1, 0))
FAR = ((1, 1), (1, -1), (-1, 1), (-1, -1), (2, 0), (-2, 0))
UNROLL = 64


def slot_list(nr, nc):
    near, slots = [], []
    for offsets, out in ((NEAR, near), (FAR, None)):
        for di, dj in offsets:
            off = (di % nr, dj % nc)
            if off not in slots:
                slots.append(off)
                if out is not None:
                    out.append(off)
    return near, slots


def kernel(nr, nc, near, slots, sc, nrhs, loads_in, cpl_in, cinv_in, part_in, linv, dirich, out,
           loads, cpl, cinv, part, lbuf, dbuf, lpair, dpair, loads_n, part_n, cpl_n, kc, kt, ub, qb,
           local_sem, k_send, k_recv, c_send, c_recv, l_send, l_recv, p_send, p_recv, d_send, d_recv,
           u_send, u_recv, q_send, q_recv):
    rows, width = loads.shape
    edge = width // 4
    ndev = nr * nc
    ncols = nc * sc
    lanes = kt.shape[-1]
    i, j = lax.axis_index("srow"), lax.axis_index("scol")

    def target(di, dj):
        return (lax.rem(i - di + nr, nr), lax.rem(j - dj + nc, nc))

    def others(step):
        if ndev <= UNROLL:
            for k in range(1, ndev):
                step(k, k // nc, k % nc)
        else:
            @pl.loop(1, ndev)
            def _(k):
                step(k, lax.div(k, nc), lax.rem(k, nc))

    barrier = pltpu.get_barrier_semaphore()

    def greet(k, di, dj):
        pl.semaphore_signal(barrier, inc=1, device_id=target(di, dj), device_id_type=MESH)

    others(greet)

    fetches = [
        pltpu.make_async_copy(src, dst, local_sem.at[n])
        for n, (src, dst) in enumerate((
            (cinv_in, cinv), (loads_in, loads), (cpl_in, cpl), (part_in, part),
            (linv, lbuf), (dirich, dbuf.at[0]),
        ))
    ]
    for fetch in fetches:
        fetch.start()

    row = lax.broadcasted_iota(jnp.int32, (rows, width), 0)
    lane = lax.broadcasted_iota(jnp.int32, (rows, width), 1)
    wrow = lax.broadcasted_iota(jnp.int32, (rows, lanes), 0)
    wlane = lax.broadcasted_iota(jnp.int32, (rows, lanes), 1)
    wrhs = lax.rem(wrow, nrhs)
    wsub = lax.div(wrow, nrhs)
    of_rhs = lax.div(wlane, ncols) == wrhs
    gamma_lane = wlane == nrhs * ncols + wrhs
    curve_lane = wlane == nrhs * ncols + nrhs + wrhs

    def spread(block):
        out = jnp.broadcast_to(block[0:1], (rows, block.shape[1]))
        which = lax.div(lax.broadcasted_iota(jnp.int32, out.shape, 0), nrhs)
        for s in range(1, sc):
            out = jnp.where(which == s, jnp.broadcast_to(block[s : s + 1], out.shape), out)
        return out

    def place(dj):
        column = lax.rem(j + dj, nc) * sc
        return wlane == wrhs * ncols + column + wsub

    def index_of(block):
        partner = spread(block)
        position = jnp.clip(partner, 0, edge - 1) + (edge * (1 - 2 * lax.rem(lax.div(lane, edge), 2)) + lax.div(lane, edge) * edge)
        return position, partner >= 0

    def split(values):
        high = values.astype(jnp.bfloat16)
        return high, (values - high.astype(jnp.float32)).astype(jnp.bfloat16)

    def split_into(pair, blocks):
        for s, block in enumerate(blocks):
            high, low = split(block)
            pair[s * width : (s + 1) * width, 0:width] = high
            pair[s * width : (s + 1) * width, width : 2 * width] = low

    tile_lane = lax.broadcasted_iota(jnp.int32, (ncols, lanes), 1)
    tile_row = lax.broadcasted_iota(jnp.int32, (ncols, lanes), 0)
    tiler = jnp.where(lax.rem(tile_lane, ncols) == tile_row, 1.0, 0.0)
    for fetch in fetches[:4]:
        fetch.wait()
    tiled = jnp.dot(spread(cinv[...]), tiler, precision=precise, preferred_element_type=jnp.float32)
    for s in range(sc):
        kc[0, s : s + 1] = tiled[s * nrhs : s * nrhs + 1]
    kt[0] = jnp.where(of_rhs, tiled, 0.0)

    own_position, own_active = index_of(part[...])
    coupling = spread(cpl[...])
    own_place = place(0)
    fetches[4].wait()
    split_into(lpair, [lbuf[s] for s in range(sc)])

    pl.semaphore_wait(barrier, ndev - 1)

    def remote(src, dst, send, recv, off):
        copy = pltpu.make_async_remote_copy(
            src_ref=src, dst_ref=dst, send_sem=send, recv_sem=recv,
            device_id=target(*off), device_id_type=MESH)
        copy.start()
        return copy

    load_copies = [remote(loads, loads_n.at[n], l_send.at[n], l_recv.at[n], near[n]) for n in range(1, len(near))]
    part_copies = [remote(part, part_n.at[n], p_send.at[n], p_recv.at[n], near[n]) for n in range(1, len(near))]
    cpl_copies = [remote(cpl, cpl_n.at[n], c_send.at[n], c_recv.at[n], slots[n]) for n in range(1, len(slots))]
    east_off, west_off = (0, 1 % nc), (0, nc - 1)
    d_copies = []
    for n in range(1, len(near)):
        if near[n] == east_off:
            src, dst = dirich.at[pl.ds(0, 1)], dbuf.at[n, pl.ds(0, 1)]
        elif near[n] == west_off:
            src, dst = dirich.at[pl.ds(sc - 1, 1)], dbuf.at[n, pl.ds(sc - 1, 1)]
        else:
            src, dst = dirich, dbuf.at[n]
        d_copies.append((src, dst, d_send.at[n], d_recv.at[n], near[n]))

    def send_k(k, di, dj):
        remote(kc.at[0], kc.at[k], k_send, k_recv, (di, dj))

    others(send_k)
    d_copies = [remote(*args) for args in d_copies]

    def jump(mine, west_tile, east_tile, south, north, lookup):
        position, active = lookup
        west = jnp.where(row < nrhs, pltpu.roll(west_tile, nrhs, 0), pltpu.roll(mine, nrhs, 0))
        east = jnp.where(row >= rows - nrhs, pltpu.roll(east_tile, rows - nrhs, 0), pltpu.roll(mine, rows - nrhs, 0))
        side = lax.div(lane, edge)
        comb = jnp.where(side == 0, east, jnp.where(side == 1, west, jnp.where(side == 2, north, south)))
        facing = jnp.take_along_axis(comb, position, axis=1, mode="promise_in_bounds")
        return jnp.where(active, mine - facing, 0.0)

    def slot_of(di, dj):
        off = (di % nr, dj % nc)
        return slots.index(off) if off in slots else None

    def jump_at(tiles, di, dj, lookup):
        def tile(a, b):
            n = slot_of(a, b)
            return tiles[n] if n is not None and n in tiles else tiles[slot_of(di, dj)]
        return jump(tiles[slot_of(di, dj)], tile(di, dj - 1), tile(di, dj + 1), tile(di - 1, dj), tile(di + 1, dj), lookup)

    def multiply(values, pair, count):
        high, low = split(values)
        stacked = jnp.concatenate([high.astype(jnp.float32), low.astype(jnp.float32)], axis=0)
        sub = lax.rem(lax.div(lax.broadcasted_iota(jnp.int32, stacked.shape, 0), nrhs), sc)
        wide = jnp.concatenate(
            [jnp.where(sub == (s if s < count - 1 else sc - 1), stacked, 0.0) for s in range(count)], axis=1)
        product = jnp.dot(wide.astype(jnp.bfloat16), pair, preferred_element_type=jnp.float32)
        return (product[0:rows, 0:width] + product[rows:, 0:width]) + (product[0:rows, width:] + product[rows:, width:])

    def lane_sum(values):
        return jnp.sum(values, axis=1, keepdims=True)

    def publish(rd, values, dots, wide):
        u = multiply(values, lpair[...], sc)
        ub[rd, 0] = u
        count = len(slots) if wide else len(near)
        for n in range(1, count):
            remote(ub.at[rd, 0], ub.at[rd, n], u_send.at[rd], u_recv.at[rd], slots[n])
        message = jnp.where(own_place, lane_sum(coupling * values), 0.0)
        if dots is not None:
            gamma, factor = dots
            message = jnp.where(gamma_lane, lane_sum(gamma), message)
            message = jnp.where(curve_lane, lane_sum(factor * u), message)
        qb[rd, 0] = jnp.sum(message, axis=0, keepdims=True)

        def send_q(k, di, dj):
            remote(qb.at[rd, 0], qb.at[rd, k], q_send.at[rd], q_recv.at[rd], (di, dj))

        others(send_q)
        return count

    def collect(rd, count, want_dots):
        bytes_q = qb.at[rd, pl.ds(1, ndev - 1)]
        pltpu.make_async_copy(bytes_q, bytes_q, q_recv.at[rd]).wait()
        band = [jnp.broadcast_to(jnp.sum(qb[rd, pl.ds(d * nc, nc)], axis=0), (rows, lanes)) for d in range(nr)]
        cols = {}

        def column(k, d):
            return lane_sum(band[d] * kt[k])

        gamma = curve = None
        if want_dots:
            cross = jnp.zeros((rows, lanes), jnp.float32)
            for d in range(nr):
                total = jnp.zeros((rows, lanes), jnp.float32)
                if ndev <= UNROLL:
                    for e in range(nc):
                        cols[(d, e)] = column(d * nc + e, d)
                        total = total + jnp.where(place(e), cols[(d, e)], 0.0)
                else:
                    def add(e, total):
                        return total + jnp.where(place(e), column(d * nc + e, d), 0.0)
                    total = lax.fori_loop(0, nc, add, total)
                cross = cross + total * band[d]
            everything = functools.reduce(jnp.add, band)
            crossed = jnp.broadcast_to(jnp.sum(cross, axis=0, keepdims=True), (rows, lanes))
            curve = lane_sum(jnp.where(of_rhs, crossed, 0.0) + jnp.where(curve_lane, everything, 0.0))
            gamma = lane_sum(jnp.where(gamma_lane, everything, 0.0))
        bytes_u = ub.at[rd, pl.ds(1, count - 1)]
        pltpu.make_async_copy(bytes_u, bytes_u, u_recv.at[rd]).wait()
        tiles = {}
        for n in range(count):
            off = slots[n]
            if off not in cols:
                cols[off] = column(off[0] * nc + off[1], off[0])
            tiles[n] = ub[rd, n] + couplings[n] * cols[off]
        return tiles, gamma, curve

    for n, copy in enumerate(load_copies):
        copy.wait_recv()
    own_lookup = (own_position, own_active)
    load_tiles = {n: (loads[...] if n == 0 else loads_n[n]) for n in range(len(near))}
    start = jump_at(load_tiles, 0, 0, own_lookup)
    count = publish(0, start, None, True)

    for copy in part_copies:
        copy.wait_recv()
    for copy in cpl_copies:
        copy.wait_recv()
    lookups = [own_lookup] + [index_of(part_n[n]) for n in range(1, len(near))]
    couplings = [coupling] + [spread(cpl_n[n]) for n in range(1, len(slots))]
    bytes_k = kc.at[pl.ds(1, ndev - 1)]
    pltpu.make_async_copy(bytes_k, bytes_k, k_recv).wait()

    def widen(k, di, dj):
        kt[k] = jnp.where(of_rhs, spread(kc[k]), 0.0)

    others(widen)
    fetches[5].wait()
    for copy in d_copies:
        copy.wait_recv()
    east, west = near.index(east_off), near.index(west_off)
    upright = [n for n in range(len(near)) if n not in (east, west)]
    for n in upright:
        split_into(dpair.at[n], [dbuf[n, s] for s in range(sc)])
    split_into(dpair.at[east], [dbuf[east, 0], dbuf[west, sc - 1]])
    tiles, _, _ = collect(0, count, False)
    residual = [jump_at(tiles, *near[n], lookups[n]) for n in range(len(near))]

    multipliers = jnp.zeros((rows, width), jnp.float32)
    search = along = gamma = step_size = None
    for iteration in range(ITERS):
        rd = iteration + 1
        last = rd == ITERS
        weighted = {}
        for n in upright:
            weighted[n] = multiply(2.0 * residual[n], dpair[n], sc)
        beside = jnp.where(row < nrhs, residual[east], residual[west])
        weighted[east] = weighted[west] = multiply(2.0 * beside, dpair[east, pl.ds(0, 2 * width)], 2)
        precon = jump_at(weighted, 0, 0, own_lookup)
        doubled = 2.0 * precon
        count = publish(rd, doubled, (residual[0] * precon, doubled), not last)
        tiles, gamma_new, curve = collect(rd, count, True)
        kept = 1 if last else len(near)
        image = [jump_at(tiles, *near[n], lookups[n]) for n in range(kept)]
        if iteration == 0:
            step_size = gamma_new / curve
            search, along = precon, image
        else:
            ratio = gamma_new / gamma
            step_size = gamma_new / (curve - ratio * gamma_new / step_size)
            search = precon + ratio * search
            along = [image[n] + ratio * along[n] for n in range(kept)]
        gamma = gamma_new
        multipliers = multipliers + step_size * search
        residual = [residual[n] - step_size * along[n] for n in range(kept)]
    out[0] = multipliers
    out[1] = residual[0]

    for copy in load_copies + part_copies + cpl_copies + d_copies:
        copy.wait_send()
    pltpu.make_async_copy(bytes_k, bytes_k, k_send).wait()
    for rd in range(ITERS + 1):
        bytes_q = qb.at[rd, pl.ds(1, ndev - 1)]
        pltpu.make_async_copy(bytes_q, bytes_q, q_send.at[rd]).wait()
        sent = (len(near) if rd == ITERS else len(slots)) - 1
        bytes_u = ub.at[rd, pl.ds(1, sent)]
        pltpu.make_async_copy(bytes_u, bytes_u, u_send.at[rd]).wait()


def solution(mesh):
    nr, nc = mesh.shape["srow"], mesh.shape["scol"]
    near, slots = slot_list(nr, nc)

    def body(loads, local_inverse, dirichlet, corner_coupling, coarse_inverse, partner):
        sr, sc, nrhs, width = loads.shape
        rows = sr * sc * nrhs
        ndev = nr * nc
        lanes = -(-(nrhs * nc * sc + 2 * nrhs) // 128) * 128
        dma = pltpu.SemaphoreType.DMA
        f32 = jnp.float32
        vmem = pl.BlockSpec(memory_space=pltpu.VMEM)
        hbm = pl.BlockSpec(memory_space=pl.ANY)
        rounds = ITERS + 1
        out = pl.pallas_call(
            functools.partial(kernel, nr, nc, near, slots, sc, nrhs),
            out_shape=jax.ShapeDtypeStruct((2, rows, width), f32),
            in_specs=[hbm] * 6,
            out_specs=vmem,
            scratch_shapes=[
                pltpu.VMEM((rows, width), f32),
                pltpu.VMEM((sc, width), f32),
                pltpu.VMEM((sc, coarse_inverse.shape[-1]), f32),
                pltpu.VMEM((sc, width), jnp.int32),
                pltpu.VMEM((sc, width, width), f32),
                pltpu.VMEM((len(near), sc, width, width), f32),
                pltpu.VMEM((sc * width, 2 * width), jnp.bfloat16),
                pltpu.VMEM((len(near), sc * width, 2 * width), jnp.bfloat16),
                pltpu.VMEM((len(near), rows, width), f32),
                pltpu.VMEM((len(near), sc, width), jnp.int32),
                pltpu.VMEM((len(slots), sc, width), f32),
                pltpu.VMEM((ndev, sc, lanes), f32),
                pltpu.VMEM((ndev, rows, lanes), f32),
                pltpu.VMEM((rounds, len(slots), rows, width), f32),
                pltpu.VMEM((rounds, ndev, 1, lanes), f32),
                dma((6,)), dma, dma,
                dma((len(slots),)), dma((len(slots),)),
                dma((len(near),)), dma((len(near),)),
                dma((len(near),)), dma((len(near),)),
                dma((len(near),)), dma((len(near),)),
                dma((rounds,)), dma((rounds,)),
                dma((rounds,)), dma((rounds,)),
            ],
            compiler_params=pltpu.CompilerParams(collective_id=0, has_side_effects=True),
        )(
            loads.reshape(rows, width),
            corner_coupling.reshape(sc, width),
            coarse_inverse.reshape(sc, coarse_inverse.shape[-1]),
            partner.reshape(sc, width),
            local_inverse.reshape(sc, width, width),
            dirichlet.reshape(sc, width, width),
        )
        return out[0].reshape(loads.shape), out[1].reshape(loads.shape)

    return jax.shard_map(
        body,
        mesh=mesh,
        in_specs=(
            P("srow", "scol", None, None),
            P("srow", "scol", None, None),
            P("srow", "scol", None, None),
            P("srow", "scol", None),
            P("srow", "scol", None),
            P("srow", "scol", None),
        ),
        out_specs=(P("srow", "scol", None, None), P("srow", "scol", None, None)),
        check_vma=False,
    )
```

```python
import functools

import jax
import jax.numpy as jnp
from jax import lax
from jax.experimental import pallas as pl
from jax.experimental.pallas import tpu as pltpu
from jax.sharding import PartitionSpec as P

ITERS = 3
MESH = pl.DeviceIdType.MESH
precise = lax.Precision.HIGHEST
NEAR = ((0, 0), (0, 1), (0, -1), (1, 0), (-1, 0))
FAR = ((1, 1), (1, -1), (-1, 1), (-1, -1), (2, 0), (-2, 0))
UNROLL = 64


def slot_list(nr, nc):
    near, slots = [], []
    for offsets, out in ((NEAR, near), (FAR, None)):
        for di, dj in offsets:
            off = (di % nr, dj % nc)
            if off not in slots:
                slots.append(off)
                if out is not None:
                    out.append(off)
    return near, slots


def kernel(nr, nc, near, slots, sc, nrhs, loads_in, cpl_in, cinv_in, part_in, linv, dirich, out,
           loads, cpl, cinv, part, lbuf, dbuf, lpair, dpair, loads_n, part_n, cpl_n, dnear, kc, kt, ub, qb,
           local_sem, k_send, k_recv, c_send, c_recv, l_send, l_recv, p_send, p_recv, d_send, d_recv,
           u_send, u_recv, q_send, q_recv):
    rows, width = loads.shape
    edge = width // 4
    ndev = nr * nc
    ncols = nc * sc
    lanes = kt.shape[-1]
    i, j = lax.axis_index("srow"), lax.axis_index("scol")

    def target(di, dj):
        return (lax.rem(i - di + nr, nr), lax.rem(j - dj + nc, nc))

    def others(step):
        if ndev <= UNROLL:
            far_first = sorted(range(1, ndev), key=lambda k: (-min(k // nc, nr - k // nc), min(k % nc, nc - k % nc) % (nc // 2)))
            for k in far_first:
                step(k, k // nc, k % nc)
        else:
            @pl.loop(1, ndev)
            def _(k):
                step(k, lax.div(k, nc), lax.rem(k, nc))

    barrier = pltpu.get_barrier_semaphore()

    def greet(k, di, dj):
        pl.semaphore_signal(barrier, inc=1, device_id=target(di, dj), device_id_type=MESH)

    others(greet)

    fetches = [
        pltpu.make_async_copy(src, dst, local_sem.at[n])
        for n, (src, dst) in enumerate((
            (cinv_in, cinv), (loads_in, loads), (cpl_in, cpl), (part_in, part),
            (linv, lbuf), (dirich, dbuf),
        ))
    ]
    for fetch in fetches:
        fetch.start()

    row = lax.broadcasted_iota(jnp.int32, (rows, width), 0)
    lane = lax.broadcasted_iota(jnp.int32, (rows, width), 1)
    wrow = lax.broadcasted_iota(jnp.int32, (rows, lanes), 0)
    wlane = lax.broadcasted_iota(jnp.int32, (rows, lanes), 1)
    wrhs = lax.rem(wrow, nrhs)
    wsub = lax.div(wrow, nrhs)
    of_rhs = lax.div(wlane, ncols) == wrhs
    gamma_lane = wlane == nrhs * ncols + wrhs
    curve_lane = wlane == nrhs * ncols + nrhs + wrhs

    def spread(block):
        out = jnp.broadcast_to(block[0:1], (rows, block.shape[1]))
        which = lax.div(lax.broadcasted_iota(jnp.int32, out.shape, 0), nrhs)
        for s in range(1, sc):
            out = jnp.where(which == s, jnp.broadcast_to(block[s : s + 1], out.shape), out)
        return out

    def place(dj):
        column = lax.rem(j + dj, nc) * sc
        return wlane == wrhs * ncols + column + wsub

    def index_of(block):
        partner = spread(block)
        position = jnp.clip(partner, 0, edge - 1) + (edge * (1 - 2 * lax.rem(lax.div(lane, edge), 2)) + lax.div(lane, edge) * edge)
        return position, partner >= 0

    def split(values):
        high = values.astype(jnp.bfloat16)
        return high, (values - high.astype(jnp.float32)).astype(jnp.bfloat16)

    def split_into(pair, blocks):
        for s, block in enumerate(blocks):
            high, low = split(block)
            pair[s * width : (s + 1) * width, 0:width] = high
            pair[s * width : (s + 1) * width, width : 2 * width] = low

    tile_lane = lax.broadcasted_iota(jnp.int32, (ncols, lanes), 1)
    tile_row = lax.broadcasted_iota(jnp.int32, (ncols, lanes), 0)
    tiler = jnp.where(lax.rem(tile_lane, ncols) == tile_row, 1.0, 0.0)
    for fetch in fetches[:4]:
        fetch.wait()
    tiled = jnp.dot(spread(cinv[...]), tiler, precision=precise, preferred_element_type=jnp.float32)
    for s in range(sc):
        kc[0, s : s + 1] = tiled[s * nrhs : s * nrhs + 1]
    kt[0] = jnp.where(of_rhs, tiled, 0.0)

    own_position, own_active = index_of(part[...])
    coupling = spread(cpl[...])
    own_place = place(0)
    fetches[4].wait()
    split_into(lpair, [lbuf[s] for s in range(sc)])
    for n in range(1, len(near)):
        dpair[n] = jnp.zeros(dpair.shape[1:], jnp.bfloat16)

    pl.semaphore_wait(barrier, ndev - 1)

    def remote(src, dst, send, recv, off):
        copy = pltpu.make_async_remote_copy(
            src_ref=src, dst_ref=dst, send_sem=send, recv_sem=recv,
            device_id=target(*off), device_id_type=MESH)
        copy.start()
        return copy

    load_copies = [remote(loads, loads_n.at[n], l_send.at[n], l_recv.at[n], near[n]) for n in range(1, len(near))]
    part_copies = [remote(part, part_n.at[n], p_send.at[n], p_recv.at[n], near[n]) for n in range(1, len(near))]
    cpl_copies = [remote(cpl, cpl_n.at[n], c_send.at[n], c_recv.at[n], slots[n]) for n in range(1, len(slots))]
    east_off, west_off = (0, 1 % nc), (0, nc - 1)
    facing_start = {east_off: 0, west_off: edge, (1 % nr, 0): 2 * edge, (nr - 1, 0): 3 * edge}
    d_copies = []
    for n in range(1, len(near)):
        subs = {east_off: pl.ds(0, 1), west_off: pl.ds(sc - 1, 1)}.get(near[n], pl.ds(0, sc))
        src = dirich.at[subs, pl.ds(facing_start[near[n]], edge)]
        d_copies.append((src, dnear.at[n, subs], d_send.at[n], d_recv.at[n], near[n]))

    def send_k(k, di, dj):
        remote(kc.at[0], kc.at[k], k_send, k_recv, (di, dj))

    others(send_k)
    d_copies = [remote(*args) for args in d_copies]

    def jump(mine, west_tile, east_tile, south, north, lookup):
        position, active = lookup
        west = jnp.where(row < nrhs, pltpu.roll(west_tile, nrhs, 0), pltpu.roll(mine, nrhs, 0))
        east = jnp.where(row >= rows - nrhs, pltpu.roll(east_tile, rows - nrhs, 0), pltpu.roll(mine, rows - nrhs, 0))
        side = lax.div(lane, edge)
        comb = jnp.where(side == 0, east, jnp.where(side == 1, west, jnp.where(side == 2, north, south)))
        facing = jnp.take_along_axis(comb, position, axis=1, mode="promise_in_bounds")
        return jnp.where(active, mine - facing, 0.0)

    def slot_of(di, dj):
        off = (di % nr, dj % nc)
        return slots.index(off) if off in slots else None

    def jump_at(tiles, di, dj, lookup):
        def tile(a, b):
            n = slot_of(a, b)
            return tiles[n] if n is not None and n in tiles else tiles[slot_of(di, dj)]
        return jump(tiles[slot_of(di, dj)], tile(di, dj - 1), tile(di, dj + 1), tile(di - 1, dj), tile(di + 1, dj), lookup)

    def multiply(values, pair, count):
        high, low = split(values)
        stacked = jnp.concatenate([high.astype(jnp.float32), low.astype(jnp.float32)], axis=0)
        sub = lax.rem(lax.div(lax.broadcasted_iota(jnp.int32, stacked.shape, 0), nrhs), sc)
        wide = jnp.concatenate(
            [jnp.where(sub == (s if s < count - 1 else sc - 1), stacked, 0.0) for s in range(count)], axis=1)
        product = jnp.dot(wide.astype(jnp.bfloat16), pair, preferred_element_type=jnp.float32)
        return (product[0:rows, 0:width] + product[rows:, 0:width]) + (product[0:rows, width:] + product[rows:, width:])

    def lane_sum(values):
        return jnp.sum(values, axis=1, keepdims=True)

    def publish(rd, values, dots, wide):
        u = multiply(values, lpair[...], sc)
        ub[rd, 0] = u
        count = len(slots) if wide else len(near)
        for n in range(1, count):
            remote(ub.at[rd, 0], ub.at[rd, n], u_send.at[rd], u_recv.at[rd], slots[n])
        message = jnp.where(own_place, lane_sum(coupling * values), 0.0)
        if dots is not None:
            gamma, factor = dots
            message = jnp.where(gamma_lane, lane_sum(gamma), message)
            message = jnp.where(curve_lane, lane_sum(factor * u), message)
        qb[rd, 0] = jnp.sum(message, axis=0, keepdims=True)

        def send_q(k, di, dj):
            remote(qb.at[rd, 0], qb.at[rd, k], q_send.at[rd], q_recv.at[rd], (di, dj))

        others(send_q)
        return count

    def collect(rd, count, want_dots):
        bytes_q = qb.at[rd, pl.ds(1, ndev - 1)]
        pltpu.make_async_copy(bytes_q, bytes_q, q_recv.at[rd]).wait()
        band = [jnp.broadcast_to(jnp.sum(qb[rd, pl.ds(d * nc, nc)], axis=0), (rows, lanes)) for d in range(nr)]
        cols = {}

        def column(k, d):
            return lane_sum(band[d] * kt[k])

        gamma = curve = None
        if want_dots:
            cross = jnp.zeros((rows, lanes), jnp.float32)
            for d in range(nr):
                total = jnp.zeros((rows, lanes), jnp.float32)
                if ndev <= UNROLL:
                    for e in range(nc):
                        cols[(d, e)] = column(d * nc + e, d)
                        total = total + jnp.where(place(e), cols[(d, e)], 0.0)
                else:
                    def add(e, total):
                        return total + jnp.where(place(e), column(d * nc + e, d), 0.0)
                    total = lax.fori_loop(0, nc, add, total)
                cross = cross + total * band[d]
            everything = functools.reduce(jnp.add, band)
            crossed = jnp.broadcast_to(jnp.sum(cross, axis=0, keepdims=True), (rows, lanes))
            curve = lane_sum(jnp.where(of_rhs, crossed, 0.0) + jnp.where(curve_lane, everything, 0.0))
            gamma = lane_sum(jnp.where(gamma_lane, everything, 0.0))
        bytes_u = ub.at[rd, pl.ds(1, count - 1)]
        pltpu.make_async_copy(bytes_u, bytes_u, u_recv.at[rd]).wait()
        tiles = {}
        for n in range(count):
            off = slots[n]
            if off not in cols:
                cols[off] = column(off[0] * nc + off[1], off[0])
            tiles[n] = ub[rd, n] + couplings[n] * cols[off]
        return tiles, gamma, curve

    for n, copy in enumerate(load_copies):
        copy.wait_recv()
    own_lookup = (own_position, own_active)
    load_tiles = {n: (loads[...] if n == 0 else loads_n[n]) for n in range(len(near))}
    start = jump_at(load_tiles, 0, 0, own_lookup)
    count = publish(0, start, None, True)

    for copy in part_copies:
        copy.wait_recv()
    for copy in cpl_copies:
        copy.wait_recv()
    lookups = [own_lookup] + [index_of(part_n[n]) for n in range(1, len(near))]
    couplings = [coupling] + [spread(cpl_n[n]) for n in range(1, len(slots))]
    bytes_k = kc.at[pl.ds(1, ndev - 1)]
    pltpu.make_async_copy(bytes_k, bytes_k, k_recv).wait()

    def widen(k, di, dj):
        kt[k] = jnp.where(of_rhs, spread(kc[k]), 0.0)

    others(widen)
    fetches[5].wait()
    for copy in d_copies:
        copy.wait_recv()
    east, west = near.index(east_off), near.index(west_off)
    upright = [n for n in range(len(near)) if n not in (east, west)]

    def edge_into(n, s, pair, at):
        first = facing_start[near[n]]
        high, low = split(dnear[n, s].T)
        pair[at * width : (at + 1) * width, first : first + edge] = high
        pair[at * width : (at + 1) * width, width + first : width + first + edge] = low

    split_into(dpair.at[0], [dbuf[s] for s in range(sc)])
    for n in upright[1:]:
        for s in range(sc):
            edge_into(n, s, dpair.at[n], s)
    edge_into(east, 0, dpair.at[east], 0)
    edge_into(west, sc - 1, dpair.at[east], 1)
    tiles, _, _ = collect(0, count, False)
    residual = [jump_at(tiles, *near[n], lookups[n]) for n in range(len(near))]

    multipliers = jnp.zeros((rows, width), jnp.float32)
    search = along = gamma = step_size = None
    for iteration in range(ITERS):
        rd = iteration + 1
        last = rd == ITERS
        weighted = {}
        for n in upright:
            weighted[n] = multiply(2.0 * residual[n], dpair[n], sc)
        beside = jnp.where(row < nrhs, residual[east], residual[west])
        weighted[east] = weighted[west] = multiply(2.0 * beside, dpair[east, pl.ds(0, 2 * width)], 2)
        precon = jump_at(weighted, 0, 0, own_lookup)
        doubled = 2.0 * precon
        count = publish(rd, doubled, (residual[0] * precon, doubled), not last)
        tiles, gamma_new, curve = collect(rd, count, True)
        kept = 1 if last else len(near)
        image = [jump_at(tiles, *near[n], lookups[n]) for n in range(kept)]
        if iteration == 0:
            step_size = gamma_new / curve
            search, along = precon, image
        else:
            ratio = gamma_new / gamma
            step_size = gamma_new / (curve - ratio * gamma_new / step_size)
            search = precon + ratio * search
            along = [image[n] + ratio * along[n] for n in range(kept)]
        gamma = gamma_new
        multipliers = multipliers + step_size * search
        residual = [residual[n] - step_size * along[n] for n in range(kept)]
    out[0] = multipliers
    out[1] = residual[0]

    for copy in load_copies + part_copies + cpl_copies + d_copies:
        copy.wait_send()
    pltpu.make_async_copy(bytes_k, bytes_k, k_send).wait()
    for rd in range(ITERS + 1):
        bytes_q = qb.at[rd, pl.ds(1, ndev - 1)]
        pltpu.make_async_copy(bytes_q, bytes_q, q_send.at[rd]).wait()
        sent = (len(near) if rd == ITERS else len(slots)) - 1
        bytes_u = ub.at[rd, pl.ds(1, sent)]
        pltpu.make_async_copy(bytes_u, bytes_u, u_send.at[rd]).wait()


def solution(mesh):
    nr, nc = mesh.shape["srow"], mesh.shape["scol"]
    near, slots = slot_list(nr, nc)

    def body(loads, local_inverse, dirichlet, corner_coupling, coarse_inverse, partner):
        sr, sc, nrhs, width = loads.shape
        rows = sr * sc * nrhs
        ndev = nr * nc
        lanes = -(-(nrhs * nc * sc + 2 * nrhs) // 128) * 128
        dma = pltpu.SemaphoreType.DMA
        f32 = jnp.float32
        vmem = pl.BlockSpec(memory_space=pltpu.VMEM)
        hbm = pl.BlockSpec(memory_space=pl.ANY)
        rounds = ITERS + 1
        out = pl.pallas_call(
            functools.partial(kernel, nr, nc, near, slots, sc, nrhs),
            out_shape=jax.ShapeDtypeStruct((2, rows, width), f32),
            in_specs=[hbm] * 6,
            out_specs=vmem,
            scratch_shapes=[
                pltpu.VMEM((rows, width), f32),
                pltpu.VMEM((sc, width), f32),
                pltpu.VMEM((sc, coarse_inverse.shape[-1]), f32),
                pltpu.VMEM((sc, width), jnp.int32),
                pltpu.VMEM((sc, width, width), f32),
                pltpu.VMEM((sc, width, width), f32),
                pltpu.VMEM((sc * width, 2 * width), jnp.bfloat16),
                pltpu.VMEM((len(near), sc * width, 2 * width), jnp.bfloat16),
                pltpu.VMEM((len(near), rows, width), f32),
                pltpu.VMEM((len(near), sc, width), jnp.int32),
                pltpu.VMEM((len(slots), sc, width), f32),
                pltpu.VMEM((len(near), sc, width // 4, width), f32),
                pltpu.VMEM((ndev, sc, lanes), f32),
                pltpu.VMEM((ndev, rows, lanes), f32),
                pltpu.VMEM((rounds, len(slots), rows, width), f32),
                pltpu.VMEM((rounds, ndev, 1, lanes), f32),
                dma((6,)), dma, dma,
                dma((len(slots),)), dma((len(slots),)),
                dma((len(near),)), dma((len(near),)),
                dma((len(near),)), dma((len(near),)),
                dma((len(near),)), dma((len(near),)),
                dma((rounds,)), dma((rounds,)),
                dma((rounds,)), dma((rounds,)),
            ],
            compiler_params=pltpu.CompilerParams(collective_id=0, has_side_effects=True),
        )(
            loads.reshape(rows, width),
            corner_coupling.reshape(sc, width),
            coarse_inverse.reshape(sc, coarse_inverse.shape[-1]),
            partner.reshape(sc, width),
            local_inverse.reshape(sc, width, width),
            dirichlet.reshape(sc, width, width),
        )
        return out[0].reshape(loads.shape), out[1].reshape(loads.shape)

    return jax.shard_map(
        body,
        mesh=mesh,
        in_specs=(
            P("srow", "scol", None, None),
            P("srow", "scol", None, None),
            P("srow", "scol", None, None),
            P("srow", "scol", None),
            P("srow", "scol", None),
            P("srow", "scol", None),
        ),
        out_specs=(P("srow", "scol", None, None), P("srow", "scol", None, None)),
        check_vma=False,
    )
```
